32 devices in a mesh: rx: 2 (over y), ry: 4 (over z), tp: 4 (over x, core).
Axes of the slice: x: 2, y: 2, z: 4, core: 2. Of those that a mesh axis runs over, the one named last changes fastest.
Arguments:
- weight: float32 [2, 4, 96, 4096], P('rx', 'ry', 'tp'), may hold values from -6 to 6
- public: float32 [2, 4, 96, 4096], P('rx', 'ry', 'tp'), may hold values from -6 to 6
- mixture: float32 [2, 4, 96, 4096], P('rx', 'ry', 'tp'), may hold values from -6 to 6
- moment_one: float32 [2, 4, 96, 4096], P('rx', 'ry', 'tp'), may hold values from -0.6 to 0.6
- moment_two: float32 [2, 4, 96, 4096], P('rx', 'ry', 'tp'), may hold values from 0.01 to 1
- stored: bfloat16 [2, 4, 96, 1024], P('rx', 'ry', 'tp'), may hold values from -6 to 6
- out_grad: bfloat16 [2, 4, 1024, 4096], P('rx', 'ry', 'tp'), may hold values from -0.5 to 0.5
Outputs:
- weight_new: float32 [2, 4, 96, 4096], P('rx', 'ry', 'tp')
- public_new: float32 [2, 4, 96, 4096], P('rx', 'ry', 'tp')
- mixture_new: float32 [2, 4, 96, 4096], P('rx', 'ry', 'tp')
- first_new: float32 [2, 4, 96, 4096], P('rx', 'ry', 'tp')
- second_new: float32 [2, 4, 96, 4096], P('rx', 'ry', 'tp')
The draws below stay inside these ranges and needn't reach their ends.
All inputs are finite; a program needn't handle non-finite values.
Results may differ from the reference program's by a relative error of at most 0.0039.
Values may be sent and summed in bfloat16 or wider, within the bound.
No kernel may reach another device: no remote copies, remote signals or barrier semaphores. Data moves between devices by JAX's collectives and lax.ppermute only.
A program may use at most 64 MiB of HBM per device.

```python
import math
import jax
import jax.numpy as jnp

D = 4096
TOK = 1024
ROUNDS = 2
ALL_ROWS = 96
RX_REPL = 2
RY_REPL = 4


def steps_of(key, extent, shards, low, largest):
    factor_of = 1.0
    for position, blocks in shards:
        draws = jax.random.uniform(jax.random.fold_in(jax.random.fold_in(key, 6), position), (blocks,), jnp.float32, low / len(shards), largest / len(shards))
        factor_of = factor_of * jnp.repeat(jnp.exp(draws), extent[position] // blocks).reshape((-1,) + (1,) * (len(extent) - 1 - position))
    return factor_of


def centred(key, extent, width, bound, pieces=(), held_as=jnp.bfloat16):
    loudness = steps_of(key, extent, pieces, -0.22, 0.18) if pieces else 1.0
    entries = jax.random.normal(key, extent, jnp.float32) * width * loudness
    return jnp.minimum(jnp.maximum(entries, -bound), bound).astype(held_as)


def setup_inputs(seed: int = 0) -> dict:
    splits = jax.random.split(jax.random.key(seed), 8)
    return {
        "weight": centred(splits[0], (RX_REPL, RY_REPL, ALL_ROWS, D), 1.0, 6.0, ((0, 2), (1, 4), (2, 4)), jnp.float32),
        "public": centred(splits[1], (RX_REPL, RY_REPL, ALL_ROWS, D), 1.0, 6.0, ((0, 2), (1, 4), (2, 4)), jnp.float32),
        "mixture": centred(splits[2], (RX_REPL, RY_REPL, ALL_ROWS, D), 1.0, 6.0, ((0, 2), (1, 4), (2, 4)), jnp.float32),
        "moment_one": centred(splits[3], (RX_REPL, RY_REPL, ALL_ROWS, D), 0.1, 0.6, ((0, 2), (1, 4), (2, 4)), jnp.float32),
        "moment_two": jnp.clip(jnp.exp(math.log(1.0) - 4.6051702 * jax.random.uniform(splits[4], (RX_REPL, RY_REPL, ALL_ROWS, D), jnp.float32) ** steps_of(splits[4], (RX_REPL, RY_REPL, ALL_ROWS, D), ((0, 2), (1, 4), (2, 4)), -0.2, 0.2)), 0.01, 1.0),
        "stored": centred(splits[5], (RX_REPL, RY_REPL, ALL_ROWS, TOK), 1.0, 6.0, ((0, 2), (1, 4), (2, 4))),
        "out_grad": centred(splits[6], (RX_REPL, RY_REPL, TOK, D), 0.0625, 0.5, ((0, 2), (1, 4), (2, 4))),
    }


beta_one = 0.9
beta_two = 0.95
first_fix = 0.9999734386011124
second_fix = 0.994079470779666
learn_rate = 0.02
decay_rate = 0.1
epsilon = 1e-08
step_size = 0.5

def reference(weight, public, mixture, moment_one, moment_two, stored, out_grad):
    gradient = jnp.einsum('abrt,abtd->abrd', stored.astype(jnp.float32), out_grad.astype(jnp.float32))
    first_new = beta_one * moment_one + (1.0 - beta_one) * gradient
    second_new = beta_two * moment_two + (1.0 - beta_two) * gradient * gradient
    adjusted = first_new / first_fix / (jnp.sqrt(second_new / second_fix) + epsilon)
    current = weight - learn_rate * (adjusted + decay_rate * weight)
    public_new = public
    mixture_new = mixture
    for gossip_turn in range(ROUNDS):
        sent = (current - public_new).astype(jnp.bfloat16).astype(jnp.float32)
        beside_all = jnp.roll(sent, 1, 0) + jnp.roll(sent, -1, 0) + jnp.roll(sent, 1, 1) + jnp.roll(sent, -1, 1)
        public_new = public_new + sent
        mixture_new = mixture_new + (sent + beside_all) / 5.0
        current = current + step_size * (mixture_new - public_new)
    return (current, public_new, mixture_new, first_new, second_new)
```

```python
import jax
import jax.numpy as jnp
from jax import lax
from jax.sharding import PartitionSpec as P

ROUNDS = 2


beta_one = 0.9
beta_two = 0.95
first_fix = 0.9999734386011124
second_fix = 0.994079470779666
learn_rate = 0.02
decay_rate = 0.1
epsilon = 1e-08
step_size = 0.5


def passed_along(value, axis, steps):
    count = lax.axis_size(axis)
    pairs = [(source, (source + steps) % count) for source in range(count)]
    return lax.ppermute(value, axis, pairs)


def to_twin(value):
    count = lax.axis_size("tp")
    return lax.ppermute(value, "tp", [(s, s ^ 1) for s in range(count)])


def reduced_gradient(acts, grads):
    count = lax.axis_size("tp")
    me = lax.axis_index("tp")
    width = acts.shape[1] // count
    chips = count // 2
    chip, core = me // 2, me % 2

    def block_for(owner):
        return lax.dynamic_slice_in_dim(acts, owner * width, width, 1)

    def moved(value, steps, twin):
        pairs = []
        for s in range(count):
            c = s % 2
            t = ((s // 2 + steps) % chips) * 2 + (1 - c if twin else c)
            pairs.append((s, t))
        return lax.ppermute(value, "tp", pairs)

    held = {}
    for steps in list(range(1, chips)) + [0]:
        for twin in (True, False):
            owner = ((chip + steps) % chips) * 2 + (1 - core if twin else core)
            block = block_for(owner)
            if steps or twin:
                block = moved(block, steps, twin)
            held[steps, twin] = block

    def term(steps, twin):
        return jnp.dot(held[steps, twin], grads, preferred_element_type=jnp.float32)

    total = None
    for steps in list(range(1, chips)) + [0]:
        theirs = to_twin(term(steps, True))
        pair_sum = term(steps, False) + theirs
        if steps:
            pair_sum = moved(pair_sum.astype(jnp.bfloat16), -steps, False)
            pair_sum = pair_sum.astype(jnp.float32)
        total = pair_sum if total is None else total + pair_sum
    return total


def per_device(weight, public, mixture, moment_one, moment_two, stored, out_grad):
    gradient = reduced_gradient(stored[0, 0], out_grad[0, 0])
    gradient = gradient[None, None]
    first_new = beta_one * moment_one + (1.0 - beta_one) * gradient
    second_new = beta_two * moment_two + (1.0 - beta_two) * gradient * gradient
    adjusted = first_new / first_fix / (jnp.sqrt(second_new / second_fix) + epsilon)
    current = weight - learn_rate * (adjusted + decay_rate * weight)
    public_new = public
    mixture_new = mixture
    for gossip_turn in range(ROUNDS):
        sent = (current - public_new).astype(jnp.bfloat16)
        row_next = passed_along(sent, "rx", 1)
        row_prev = passed_along(sent, "rx", -1)
        col_next = passed_along(sent, "ry", 1)
        col_prev = passed_along(sent, "ry", -1)
        beside_all = (
            row_next.astype(jnp.float32)
            + row_prev.astype(jnp.float32)
            + col_next.astype(jnp.float32)
            + col_prev.astype(jnp.float32)
        )
        own_sent = sent.astype(jnp.float32)
        public_new = public_new + own_sent
        mixture_new = mixture_new + (own_sent + beside_all) / 5.0
        current = current + step_size * (mixture_new - public_new)
    return (current, public_new, mixture_new, first_new, second_new)


def solution(mesh):
    spec = P("rx", "ry", "tp", None)
    return jax.shard_map(
        per_device, mesh=mesh, in_specs=(spec,) * 7, out_specs=(spec,) * 5, check_vma=False
    )
```
